32 devices in a mesh: aa: 4 (over z), ba: 8 (over y, x, core).
Axes of the slice: x: 2, y: 2, z: 4, core: 2. Of those that a mesh axis runs over, the one named last changes fastest.
Arguments:
- grad_out: bfloat16 [4096, 4096], P('aa', 'ba')
- saved_input: bfloat16 [4096, 4096], P(('aa', 'ba'))
- keep_bits: int32 [4096, 128], P(('aa', 'ba')), may hold values from -2147483648 to 2147483647, as said below
- gain: float32 [4096], replicated, may hold values from 0.5 to 1.5
Outputs:
- grad_in: bfloat16 [4096, 4096], P(('aa', 'ba'))
- gain_grad: float32 [4096], P('ba')
The draws below stay inside these ranges and needn't reach their ends.
Inputs may be any that keep to these rules, and one draw needn't show every extreme that they name: `keep_bits`: bit k of word w in row t (bit 31 being the sign bit) is the keep flag of feature 32 * w + k of token t; about nine in ten flags are 1.
All inputs are finite; a program needn't handle non-finite values.
Results may differ from the reference program's by a relative error of at most 0.001.
Values may be sent and summed in bfloat16 or wider, within the bound.
A program may use at most 64 MiB of HBM per device.

```python
import math
import jax
import jax.numpy as jnp
from jax import lax

D = 4096
TOKENS = 4096
WORDS = 128


def draw_grad_out(key, part):
    first = jax.random.fold_in(key, 11)
    second = jax.random.fold_in(key, 12)
    rise = 1.0 + 2.0 * jnp.arange(TOKENS, dtype=jnp.float32) / TOKENS
    rough = jnp.exp(jax.random.uniform(second, (TOKENS,), jnp.float32, jnp.log(0.5), jnp.log(2.0)))
    base = jax.random.normal(first, (TOKENS, D), jnp.float32)
    values = base * (rise * rough)[:, None]
    return values.astype(jnp.bfloat16)


def draw_saved_input(key, part):
    first = jax.random.fold_in(key, 21)
    second = jax.random.fold_in(key, 22)
    third = jax.random.fold_in(key, 23)
    base = jax.random.normal(first, (TOKENS, D), jnp.float32)
    row_scale = jnp.exp(jax.random.uniform(second, (TOKENS,), jnp.float32, jnp.log(0.3), jnp.log(3.0)))
    column_scale = jnp.exp(jax.random.uniform(third, (D,), jnp.float32, jnp.log(0.5), jnp.log(5.0)))
    values = base * row_scale[:, None] * column_scale[None, :]
    return values.astype(jnp.bfloat16)


def draw_keep_bits(key, part):
    picks = jax.random.randint(jax.random.fold_in(key, 31), (TOKENS, WORDS, 32), 0, 10)
    flags = (picks < 9).astype(jnp.int32)
    shifts = jnp.arange(32, dtype=jnp.int32)
    return jnp.sum(jnp.left_shift(flags, shifts[None, None, :]), axis=-1).astype(jnp.int32)


def setup_inputs(seed: int = 0) -> dict:
    seeds = jax.random.split(jax.random.key(seed), 5)
    grad_out = draw_grad_out(jax.random.fold_in(seeds[4], 71), 0)
    saved_input = draw_saved_input(jax.random.fold_in(seeds[4], 71), 0)
    keep_bits = draw_keep_bits(jax.random.fold_in(seeds[4], 71), 0)
    gain = jnp.clip(1.0 + 0.1 * jax.random.normal(seeds[3], (D,), jnp.float32), 0.5, 1.5)
    return {"grad_out": grad_out, "saved_input": saved_input, "keep_bits": keep_bits, "gain": gain}


KEEP_RATE = 0.9
EPSILON = 1e-06

def unpack_bits(words):
    shifts = jnp.arange(32, dtype=jnp.int32)
    bits = jnp.right_shift(words[:, :, None], shifts[None, None, :]) & 1
    return bits.reshape(words.shape[0], words.shape[1] * 32).astype(jnp.float32)

def rows_backward(grad_rows, input_rows, word_rows, gain):
    keep = unpack_bits(word_rows)
    dropped = input_rows.astype(jnp.float32) * keep * (1.0 / KEEP_RATE)
    inverse = lax.rsqrt(lax.optimization_barrier(jnp.mean(dropped * dropped, axis=-1, keepdims=True)) + EPSILON)
    normed = dropped * inverse
    grads = grad_rows.astype(jnp.float32)
    scaled = gain[None, :] * grads
    centre = lax.optimization_barrier(jnp.mean(scaled * normed, axis=-1, keepdims=True))
    grad_in = (inverse * (scaled - normed * centre) * keep * (1.0 / KEEP_RATE)).astype(jnp.bfloat16)
    partial_sum = lax.optimization_barrier(jnp.sum(grads * normed, axis=0))
    return (grad_in, partial_sum)

def reference(grad_out, saved_input, keep_bits, gain):
    block = math.gcd(TOKENS, 512)
    count = TOKENS // block

    def one_block(items):
        return rows_backward(items[0], items[1], items[2], gain)
    grad_in, partial_sums = lax.map(one_block, (grad_out.reshape(count, block, D), saved_input.reshape(count, block, D), keep_bits.reshape(count, block, WORDS)))
    gain_grad = lax.optimization_barrier(jnp.sum(partial_sums, axis=0)) * (1.0 / math.sqrt(TOKENS))
    return (grad_in.reshape(TOKENS, D), gain_grad)
```

```python
import functools
import math

import jax
import jax.numpy as jnp
from jax import lax
from jax.experimental import pallas as pl
from jax.experimental.pallas import tpu as pltpu
from jax.sharding import PartitionSpec as P

KEEP_RATE = 0.9
EPSILON = 1e-06
LANES = 128
CHUNK_ROWS = 32
MESH = pl.DeviceIdType.MESH


def unpack_bits(words):
    shifts = jnp.arange(32, dtype=jnp.int32)
    bits = jnp.right_shift(words[:, :, None], shifts[None, None, :]) & 1
    return bits.reshape(words.shape[0], words.shape[1] * 32).astype(jnp.float32)


def rows_backward(grad_rows, input_rows, word_rows, gain):
    keep = unpack_bits(word_rows)
    dropped = input_rows.astype(jnp.float32) * keep * (1.0 / KEEP_RATE)
    inverse = lax.rsqrt(jnp.mean(dropped * dropped, axis=-1, keepdims=True) + EPSILON)
    normed = dropped * inverse
    grads = grad_rows.astype(jnp.float32)
    scaled = gain[None, :] * grads
    centre = jnp.mean(scaled * normed, axis=-1, keepdims=True)
    grad_in = (inverse * (scaled - normed * centre) * keep * (1.0 / KEEP_RATE)).astype(jnp.bfloat16)
    partial_sum = jnp.sum(grads * normed, axis=0)
    return (grad_in, partial_sum)


def plain(grad_out, saved_input, keep_bits, gain):
    groups = lax.axis_size("ba")
    rows = grad_out.shape[0] // groups
    pieces = grad_out.reshape(groups, rows, grad_out.shape[1])
    arrived = lax.all_to_all(pieces, "ba", split_axis=0, concat_axis=2, tiled=True)
    grad_rows = arrived.reshape(rows, arrived.shape[2])
    grad_in, partial_sum = rows_backward(grad_rows, saved_input, keep_bits, gain)
    total_tokens = rows * groups * lax.axis_size("aa")
    owned = lax.psum_scatter(partial_sum, "ba", scatter_dimension=0, tiled=True)
    share = lax.psum(owned, "aa")
    gain_grad = share * (1.0 / math.sqrt(total_tokens))
    return (grad_in, gain_grad)


def kernel(n_ba, n_aa, grad_hbm, input_hbm, bits_hbm, gain_hbm, out_ref, share_ref,
           arrived, held, words, gain_ref, normed, masked_gain, outer, sums,
           parts, slices, shares, send_sem, recv_sem, own_sem, load_sem,
           part_send, part_recv, share_send, share_recv):
    ba, aa = lax.axis_index("ba"), lax.axis_index("aa")
    rows, width = arrived.shape[1], arrived.shape[2]
    depth = n_ba * width
    chunks = rows // CHUNK_ROWS
    tiles = width // LANES
    power = n_ba & (n_ba - 1) == 0

    def ba_peer(step):
        return ba ^ step if power else lax.rem(ba + step, n_ba)

    def ba_source(step):
        return ba ^ step if power else lax.rem(ba + n_ba - step, n_ba)

    def aa_peer(step):
        return lax.rem(aa + step, n_aa)

    def piece(chunk, step):
        peer = ba_peer(step)
        first = pl.multiple_of(peer * rows + chunk * CHUNK_ROWS, CHUNK_ROWS)
        return pltpu.make_async_remote_copy(
            src_ref=grad_hbm.at[pl.ds(first, CHUNK_ROWS)],
            dst_ref=arrived.at[ba, pl.ds(chunk * CHUNK_ROWS, CHUNK_ROWS)],
            send_sem=send_sem.at[chunk, step],
            recv_sem=recv_sem.at[chunk, step],
            device_id={"ba": peer},
            device_id_type=MESH,
        )

    barrier = pltpu.get_barrier_semaphore()
    for step in range(1, n_ba):
        pl.semaphore_signal(barrier, inc=1, device_id={"ba": ba_peer(step)}, device_id_type=MESH)
    for step in range(1, n_aa):
        pl.semaphore_signal(barrier, inc=1, device_id={"aa": aa_peer(step)}, device_id_type=MESH)
    loads = [
        pltpu.make_async_copy(bits_hbm, words, load_sem.at[0]),
        pltpu.make_async_copy(gain_hbm, gain_ref, load_sem.at[1]),
        pltpu.make_async_copy(input_hbm, held, load_sem.at[2]),
    ]
    own = pltpu.make_async_copy(
        grad_hbm.at[pl.ds(pl.multiple_of(ba * rows, CHUNK_ROWS), rows)], arrived.at[ba], own_sem
    )
    for load in loads:
        load.start()
    own.start()
    pl.semaphore_wait(barrier, n_ba + n_aa - 2)
    for chunk in range(chunks):
        for step in reversed(range(1, n_ba)):
            piece(chunk, step).start()
    for load in loads:
        load.wait()

    lane = lax.broadcasted_iota(jnp.int32, (CHUNK_ROWS, LANES), 1)
    word_of = lane // 32
    flag = jnp.left_shift(jnp.int32(1), lane % 32)

    def span(source, tile):
        return pl.ds(pl.multiple_of(source * width + tile * LANES, LANES), LANES)

    def prepare(chunk, carry):
        block = pl.ds(pl.multiple_of(chunk * CHUNK_ROWS, CHUNK_ROWS), CHUNK_ROWS)

        def drop(source, squares):
            row_words = words[block, :]
            for tile in range(tiles):
                at = span(source, tile)
                index = word_of + (source * tiles + tile) * (LANES // 32)
                spread = jnp.take_along_axis(row_words, index, axis=1, mode="promise_in_bounds")
                kept = (spread & flag) != 0
                dropped = jnp.where(kept, held[block, at].astype(jnp.float32), 0.0) * (1.0 / KEEP_RATE)
                normed[block, at] = dropped
                masked_gain[block, at] = jnp.where(kept, gain_ref[:, at], 0.0)
                squares = squares + dropped * dropped
            return squares

        squares = lax.fori_loop(0, n_ba, drop, jnp.zeros((CHUNK_ROWS, LANES), jnp.float32))
        mean = jnp.sum(squares, axis=1, keepdims=True) * (1.0 / depth)
        inverse = lax.rsqrt(mean + EPSILON)
        outer[block, :] = jnp.broadcast_to(inverse * (1.0 / KEEP_RATE), (CHUNK_ROWS, LANES))

        def scale(source, none):
            for tile in range(tiles):
                at = span(source, tile)
                normed[block, at] = normed[block, at] * inverse
            return none

        lax.fori_loop(0, n_ba, scale, 0)
        return carry

    lax.fori_loop(0, chunks, prepare, 0)
    sums[...] = jnp.zeros_like(sums)
    own.wait()

    def arrive(chunk):
        block = pl.ds(pl.multiple_of(chunk * CHUNK_ROWS, CHUNK_ROWS), CHUNK_ROWS)
        for step in reversed(range(1, n_ba)):
            pltpu.make_async_remote_copy(
                src_ref=grad_hbm.at[pl.ds(0, CHUNK_ROWS)],
                dst_ref=arrived.at[ba_source(step), block],
                send_sem=send_sem.at[chunk, step],
                recv_sem=recv_sem.at[chunk, step],
                device_id={"ba": ba_peer(step)},
                device_id_type=MESH,
            ).wait_recv()

        def first(source, total):
            for tile in range(tiles):
                at = span(source, tile)
                grads = arrived[source, block, tile * LANES:(tile + 1) * LANES].astype(jnp.float32)
                product = grads * normed[block, at]
                total = total + product * gain_ref[:, at]
                sums[:, at] += jnp.sum(product.reshape(CHUNK_ROWS // 8, 8, LANES), axis=0)
            return total

        total = lax.fori_loop(0, n_ba, first, jnp.zeros((CHUNK_ROWS, LANES), jnp.float32))
        return jnp.sum(total, axis=1, keepdims=True) * (1.0 / depth)

    def finish(chunk, centre):
        block = pl.ds(pl.multiple_of(chunk * CHUNK_ROWS, CHUNK_ROWS), CHUNK_ROWS)
        factor = outer[block, :]

        def last(source, none):
            for tile in range(tiles):
                at = span(source, tile)
                grads = arrived[source, block, tile * LANES:(tile + 1) * LANES].astype(jnp.float32)
                value = factor * (masked_gain[block, at] * grads - normed[block, at] * centre)
                out_ref[block, at] = value.astype(jnp.bfloat16)
            return none

        lax.fori_loop(0, n_ba, last, 0)

    def middle(chunk, carry):
        finish(chunk, arrive(chunk))
        return carry

    lax.fori_loop(0, chunks - 1, middle, 0)
    centre = arrive(chunks - 1)
    for owner in range(n_ba):
        parts[owner] = jnp.sum(sums[:, owner * width:(owner + 1) * width], axis=0, keepdims=True)

    def part(step):
        return pltpu.make_async_remote_copy(
            src_ref=parts.at[ba_peer(step)],
            dst_ref=slices.at[ba],
            send_sem=part_send.at[step],
            recv_sem=part_recv.at[step],
            device_id={"ba": ba_peer(step)},
            device_id_type=MESH,
        )

    for step in reversed(range(1, n_ba)):
        part(step).start()
    slices[ba] = parts[ba]
    finish(chunks - 1, centre)
    for step in reversed(range(1, n_ba)):
        pltpu.make_async_remote_copy(
            src_ref=parts.at[0], dst_ref=slices.at[ba_source(step)],
            send_sem=part_send.at[step], recv_sem=part_recv.at[step],
            device_id={"ba": ba_peer(step)}, device_id_type=MESH,
        ).wait_recv()
    total = slices[0]
    for source in range(1, n_ba):
        total = total + slices[source]
    shares[aa] = total

    def share(step, slot):
        return pltpu.make_async_remote_copy(
            src_ref=shares.at[aa], dst_ref=shares.at[slot],
            send_sem=share_send.at[step], recv_sem=share_recv.at[step],
            device_id={"aa": aa_peer(step)}, device_id_type=MESH,
        )

    for step in range(1, n_aa):
        share(step, aa).start()
    for chunk in range(chunks):
        for step in range(1, n_ba):
            piece(chunk, step).wait_send()
    for step in range(1, n_ba):
        part(step).wait_send()
    for step in range(1, n_aa):
        share(step, lax.rem(aa + n_aa - step, n_aa)).wait_recv()
    total = shares[0]
    for source in range(1, n_aa):
        total = total + shares[source]
    share_ref[...] = total * (1.0 / math.sqrt(rows * n_ba * n_aa))
    for step in range(1, n_aa):
        share(step, aa).wait_send()


def fused(grad_out, saved_input, keep_bits, gain):
    n_ba, n_aa = lax.axis_size("ba"), lax.axis_size("aa")
    width = grad_out.shape[1]
    rows, depth = saved_input.shape
    chunks = rows // CHUNK_ROWS
    f32 = jnp.float32
    grad_in, share = pl.pallas_call(
        functools.partial(kernel, n_ba, n_aa),
        out_shape=(
            jax.ShapeDtypeStruct((rows, depth), jnp.bfloat16),
            jax.ShapeDtypeStruct((1, width), f32),
        ),
        in_specs=[pl.BlockSpec(memory_space=pl.ANY)] * 4,
        out_specs=(pl.BlockSpec(memory_space=pltpu.VMEM), pl.BlockSpec(memory_space=pltpu.VMEM)),
        scratch_shapes=[
            pltpu.VMEM((n_ba, rows, width), jnp.bfloat16),
            pltpu.VMEM((rows, depth), jnp.bfloat16),
            pltpu.VMEM(keep_bits.shape, jnp.int32),
            pltpu.VMEM((1, depth), f32),
            pltpu.VMEM((rows, depth), f32),
            pltpu.VMEM((rows, depth), f32),
            pltpu.VMEM((rows, LANES), f32),
            pltpu.VMEM((8, depth), f32),
            pltpu.VMEM((n_ba, 1, width), f32),
            pltpu.VMEM((n_ba, 1, width), f32),
            pltpu.VMEM((n_aa, 1, width), f32),
            pltpu.SemaphoreType.DMA((chunks, n_ba)),
            pltpu.SemaphoreType.DMA((chunks, n_ba)),
            pltpu.SemaphoreType.DMA,
            pltpu.SemaphoreType.DMA((3,)),
            pltpu.SemaphoreType.DMA((n_ba,)),
            pltpu.SemaphoreType.DMA((n_ba,)),
            pltpu.SemaphoreType.DMA((n_aa,)),
            pltpu.SemaphoreType.DMA((n_aa,)),
        ],
        compiler_params=pltpu.CompilerParams(collective_id=0, has_side_effects=True),
        name="regroup_backward",
    )(grad_out, saved_input, keep_bits, gain.reshape(1, depth))
    return (grad_in, share.reshape(width))


def per_device(grad_out, saved_input, keep_bits, gain):
    fits = grad_out.shape[1] % LANES == 0 and saved_input.shape[0] % CHUNK_ROWS == 0
    fits = fits and keep_bits.shape[1] == LANES
    body = fused if fits else plain
    return body(grad_out, saved_input, keep_bits, gain)


def solution(mesh):
    placed = (P("aa", "ba"), P(("aa", "ba"), None), P(("aa", "ba"), None), P())
    return jax.shard_map(
        per_device,
        mesh=mesh,
        in_specs=placed,
        out_specs=(P(("aa", "ba"), None), P("ba")),
        check_vma=False,
    )
```

```python
import functools
import math

import jax
import jax.numpy as jnp
from jax import lax
from jax.experimental import pallas as pl
from jax.experimental.pallas import tpu as pltpu
from jax.sharding import PartitionSpec as P

KEEP_RATE = 0.9
EPSILON = 1e-06
LANES = 128
CHUNK_ROWS = 32
STORES = 4
MESH = pl.DeviceIdType.MESH


def unpack_bits(words):
    shifts = jnp.arange(32, dtype=jnp.int32)
    bits = jnp.right_shift(words[:, :, None], shifts[None, None, :]) & 1
    return bits.reshape(words.shape[0], words.shape[1] * 32).astype(jnp.float32)


def rows_backward(grad_rows, input_rows, word_rows, gain):
    keep = unpack_bits(word_rows)
    dropped = input_rows.astype(jnp.float32) * keep * (1.0 / KEEP_RATE)
    inverse = lax.rsqrt(jnp.mean(dropped * dropped, axis=-1, keepdims=True) + EPSILON)
    normed = dropped * inverse
    grads = grad_rows.astype(jnp.float32)
    scaled = gain[None, :] * grads
    centre = jnp.mean(scaled * normed, axis=-1, keepdims=True)
    grad_in = (inverse * (scaled - normed * centre) * keep * (1.0 / KEEP_RATE)).astype(jnp.bfloat16)
    partial_sum = jnp.sum(grads * normed, axis=0)
    return (grad_in, partial_sum)


def plain(grad_out, saved_input, keep_bits, gain):
    groups = lax.axis_size("ba")
    rows = grad_out.shape[0] // groups
    pieces = grad_out.reshape(groups, rows, grad_out.shape[1])
    arrived = lax.all_to_all(pieces, "ba", split_axis=0, concat_axis=2, tiled=True)
    grad_rows = arrived.reshape(rows, arrived.shape[2])
    grad_in, partial_sum = rows_backward(grad_rows, saved_input, keep_bits, gain)
    total_tokens = rows * groups * lax.axis_size("aa")
    owned = lax.psum_scatter(partial_sum, "ba", scatter_dimension=0, tiled=True)
    share = lax.psum(owned, "aa")
    gain_grad = share * (1.0 / math.sqrt(total_tokens))
    return (grad_in, gain_grad)


def kernel(n_ba, n_aa, grad_hbm, input_hbm, bits_hbm, gain_hbm, out_ref, share_ref,
           arrived, held, words, gain_ref, normed, masked_gain, outer, sums,
           parts, slices, shares, send_sem, recv_sem, own_sem, load_sem,
           part_send, part_recv, share_send, share_recv):
    ba, aa = lax.axis_index("ba"), lax.axis_index("aa")
    rows, width = arrived.shape[1], arrived.shape[2]
    depth = n_ba * width
    chunks = rows // CHUNK_ROWS
    tiles = width // LANES
    power = n_ba & (n_ba - 1) == 0

    def ba_peer(step):
        return ba ^ step if power else lax.rem(ba + step, n_ba)

    def ba_source(step):
        return ba ^ step if power else lax.rem(ba + n_ba - step, n_ba)

    def aa_peer(step):
        return lax.rem(aa + step, n_aa)

    def piece(chunk, step):
        peer = ba_peer(step)
        first = pl.multiple_of(peer * rows + chunk * CHUNK_ROWS, CHUNK_ROWS)
        return pltpu.make_async_remote_copy(
            src_ref=grad_hbm.at[pl.ds(first, CHUNK_ROWS)],
            dst_ref=arrived.at[ba, pl.ds(chunk * CHUNK_ROWS, CHUNK_ROWS)],
            send_sem=send_sem.at[chunk, step],
            recv_sem=recv_sem.at[chunk, step],
            device_id={"ba": peer},
            device_id_type=MESH,
        )

    barrier = pltpu.get_barrier_semaphore()
    for step in range(1, n_ba):
        pl.semaphore_signal(barrier, inc=1, device_id={"ba": ba_peer(step)}, device_id_type=MESH)
    for step in range(1, n_aa):
        pl.semaphore_signal(barrier, inc=1, device_id={"aa": aa_peer(step)}, device_id_type=MESH)
    loads = [
        pltpu.make_async_copy(bits_hbm, words, load_sem.at[0]),
        pltpu.make_async_copy(gain_hbm, gain_ref, load_sem.at[1]),
        pltpu.make_async_copy(input_hbm, held, load_sem.at[2]),
    ]
    own = pltpu.make_async_copy(
        grad_hbm.at[pl.ds(pl.multiple_of(ba * rows, CHUNK_ROWS), rows)], arrived.at[ba], own_sem
    )
    for load in loads:
        load.start()
    own.start()
    pl.semaphore_wait(barrier, n_ba + n_aa - 2)
    for chunk in range(chunks):
        for step in reversed(range(1, n_ba)):
            piece(chunk, step).start()
    for load in loads:
        load.wait()

    lane = lax.broadcasted_iota(jnp.int32, (CHUNK_ROWS, LANES), 1)
    word_of = lane // 32
    flag = jnp.left_shift(jnp.int32(1), lane % 32)

    def span(source, tile):
        return pl.ds(pl.multiple_of(source * width + tile * LANES, LANES), LANES)

    def prepare(chunk, carry):
        block = pl.ds(pl.multiple_of(chunk * CHUNK_ROWS, CHUNK_ROWS), CHUNK_ROWS)

        def drop(source, squares):
            row_words = words[block, :]
            for tile in range(tiles):
                at = span(source, tile)
                index = word_of + (source * tiles + tile) * (LANES // 32)
                spread = jnp.take_along_axis(row_words, index, axis=1, mode="promise_in_bounds")
                kept = (spread & flag) != 0
                dropped = jnp.where(kept, held[block, at].astype(jnp.float32), 0.0) * (1.0 / KEEP_RATE)
                normed[block, at] = dropped
                masked_gain[block, at] = jnp.where(kept, gain_ref[:, at], 0.0)
                squares = squares + dropped * dropped
            return squares

        squares = lax.fori_loop(0, n_ba, drop, jnp.zeros((CHUNK_ROWS, LANES), jnp.float32))
        mean = jnp.sum(squares, axis=1, keepdims=True) * (1.0 / depth)
        inverse = lax.rsqrt(mean + EPSILON)
        outer[block, :] = jnp.broadcast_to(inverse * (1.0 / KEEP_RATE), (CHUNK_ROWS, LANES))

        def scale(source, none):
            for tile in range(tiles):
                at = span(source, tile)
                normed[block, at] = normed[block, at] * inverse
            return none

        lax.fori_loop(0, n_ba, scale, 0)
        return carry

    lax.fori_loop(0, chunks, prepare, 0)
    sums[...] = jnp.zeros_like(sums)
    own.wait()

    def arrive(chunk):
        block = pl.ds(pl.multiple_of(chunk * CHUNK_ROWS, CHUNK_ROWS), CHUNK_ROWS)
        for step in reversed(range(1, n_ba)):
            pltpu.make_async_remote_copy(
                src_ref=grad_hbm.at[pl.ds(0, CHUNK_ROWS)],
                dst_ref=arrived.at[ba_source(step), block],
                send_sem=send_sem.at[chunk, step],
                recv_sem=recv_sem.at[chunk, step],
                device_id={"ba": ba_peer(step)},
                device_id_type=MESH,
            ).wait_recv()

        def first(source, total):
            for tile in range(tiles):
                at = span(source, tile)
                grads = arrived[source, block, tile * LANES:(tile + 1) * LANES].astype(jnp.float32)
                product = grads * normed[block, at]
                total = total + product * gain_ref[:, at]
                sums[:, at] += jnp.sum(product.reshape(CHUNK_ROWS // 8, 8, LANES), axis=0)
            return total

        total = lax.fori_loop(0, n_ba, first, jnp.zeros((CHUNK_ROWS, LANES), jnp.float32))
        return jnp.sum(total, axis=1, keepdims=True) * (1.0 / depth)

    def finish(chunk, centre):
        block = pl.ds(pl.multiple_of(chunk * CHUNK_ROWS, CHUNK_ROWS), CHUNK_ROWS)
        factor = outer[block, :]

        def last(source, none):
            for tile in range(tiles):
                at = span(source, tile)
                grads = arrived[source, block, tile * LANES:(tile + 1) * LANES].astype(jnp.float32)
                value = factor * (masked_gain[block, at] * grads - normed[block, at] * centre)
                out_ref[block, at] = value.astype(jnp.bfloat16)
            return none

        lax.fori_loop(0, n_ba, last, 0)

    def middle(chunk, carry):
        finish(chunk, arrive(chunk))
        return carry

    lax.fori_loop(0, chunks - 1, middle, 0)
    centre = arrive(chunks - 1)
    for owner in range(n_ba):
        parts[owner] = jnp.sum(sums[:, owner * width:(owner + 1) * width], axis=0, keepdims=True)

    def part(step):
        return pltpu.make_async_remote_copy(
            src_ref=parts.at[ba_peer(step)],
            dst_ref=slices.at[ba],
            send_sem=part_send.at[step],
            recv_sem=part_recv.at[step],
            device_id={"ba": ba_peer(step)},
            device_id_type=MESH,
        )

    for step in reversed(range(1, n_ba)):
        part(step).start()
    slices[ba] = parts[ba]
    finish(chunks - 1, centre)
    for step in reversed(range(1, n_ba)):
        pltpu.make_async_remote_copy(
            src_ref=parts.at[0], dst_ref=slices.at[ba_source(step)],
            send_sem=part_send.at[step], recv_sem=part_recv.at[step],
            device_id={"ba": ba_peer(step)}, device_id_type=MESH,
        ).wait_recv()
    total = slices[0]
    for source in range(1, n_ba):
        total = total + slices[source]
    shares[aa] = total

    def share(step, slot):
        return pltpu.make_async_remote_copy(
            src_ref=shares.at[aa], dst_ref=shares.at[slot],
            send_sem=share_send.at[step], recv_sem=share_recv.at[step],
            device_id={"aa": aa_peer(step)}, device_id_type=MESH,
        )

    for step in range(1, n_aa):
        share(step, aa).start()
    for chunk in range(chunks):
        for step in range(1, n_ba):
            piece(chunk, step).wait_send()
    for step in range(1, n_ba):
        part(step).wait_send()
    for step in range(1, n_aa):
        share(step, lax.rem(aa + n_aa - step, n_aa)).wait_recv()
    total = shares[0]
    for source in range(1, n_aa):
        total = total + shares[source]
    share_ref[...] = total * (1.0 / math.sqrt(rows * n_ba * n_aa))
    for step in range(1, n_aa):
        share(step, aa).wait_send()


def store(grad_vmem, share_vmem, grad_hbm, share_hbm, sem):
    rows = grad_vmem.shape[0] // STORES
    copies = [pltpu.make_async_copy(share_vmem, share_hbm, sem.at[STORES])]
    for index in range(STORES):
        block = pl.ds(index * rows, rows)
        copies.append(pltpu.make_async_copy(grad_vmem.at[block], grad_hbm.at[block], sem.at[index]))
    for copy in copies:
        copy.start()
    for copy in copies:
        copy.wait()


def fused(grad_out, saved_input, keep_bits, gain):
    n_ba, n_aa = lax.axis_size("ba"), lax.axis_size("aa")
    width = grad_out.shape[1]
    rows, depth = saved_input.shape
    chunks = rows // CHUNK_ROWS
    f32 = jnp.float32
    grad_in, share = pl.pallas_call(
        functools.partial(kernel, n_ba, n_aa),
        out_shape=(
            pltpu.VMEM((rows, depth), jnp.bfloat16),
            pltpu.VMEM((1, width), f32),
        ),
        in_specs=[pl.BlockSpec(memory_space=pl.ANY)] * 4,
        out_specs=(pl.BlockSpec(memory_space=pltpu.VMEM), pl.BlockSpec(memory_space=pltpu.VMEM)),
        scratch_shapes=[
            pltpu.VMEM((n_ba, rows, width), jnp.bfloat16),
            pltpu.VMEM((rows, depth), jnp.bfloat16),
            pltpu.VMEM(keep_bits.shape, jnp.int32),
            pltpu.VMEM((1, depth), f32),
            pltpu.VMEM((rows, depth), f32),
            pltpu.VMEM((rows, depth), f32),
            pltpu.VMEM((rows, LANES), f32),
            pltpu.VMEM((8, depth), f32),
            pltpu.VMEM((n_ba, 1, width), f32),
            pltpu.VMEM((n_ba, 1, width), f32),
            pltpu.VMEM((n_aa, 1, width), f32),
            pltpu.SemaphoreType.DMA((chunks, n_ba)),
            pltpu.SemaphoreType.DMA((chunks, n_ba)),
            pltpu.SemaphoreType.DMA,
            pltpu.SemaphoreType.DMA((3,)),
            pltpu.SemaphoreType.DMA((n_ba,)),
            pltpu.SemaphoreType.DMA((n_ba,)),
            pltpu.SemaphoreType.DMA((n_aa,)),
            pltpu.SemaphoreType.DMA((n_aa,)),
        ],
        compiler_params=pltpu.CompilerParams(collective_id=0, has_side_effects=True),
        name="regroup_backward",
    )(grad_out, saved_input, keep_bits, gain.reshape(1, depth))
    grad_in, share = pl.pallas_call(
        store,
        out_shape=(
            jax.ShapeDtypeStruct((rows, depth), jnp.bfloat16),
            jax.ShapeDtypeStruct((1, width), f32),
        ),
        in_specs=[pl.BlockSpec(memory_space=pltpu.VMEM)] * 2,
        out_specs=[pl.BlockSpec(memory_space=pl.ANY)] * 2,
        scratch_shapes=[pltpu.SemaphoreType.DMA((STORES + 1,))],
        name="store_results",
    )(*(pltpu.with_memory_space_constraint(x, pltpu.VMEM) for x in (grad_in, share)))
    return (grad_in, share.reshape(width))


def per_device(grad_out, saved_input, keep_bits, gain):
    fits = grad_out.shape[1] % LANES == 0 and saved_input.shape[0] % CHUNK_ROWS == 0
    fits = fits and keep_bits.shape[1] == LANES
    body = fused if fits else plain
    return body(grad_out, saved_input, keep_bits, gain)


def solution(mesh):
    placed = (P("aa", "ba"), P(("aa", "ba"), None), P(("aa", "ba"), None), P())
    return jax.shard_map(
        per_device,
        mesh=mesh,
        in_specs=placed,
        out_specs=(P(("aa", "ba"), None), P("ba")),
        check_vma=False,
    )
```

```python
import functools
import math

import jax
import jax.numpy as jnp
from jax import lax
from jax.experimental import pallas as pl
from jax.experimental.pallas import tpu as pltpu
from jax.sharding import PartitionSpec as P

KEEP_RATE = 0.9
EPSILON = 1e-06
LANES = 128
CHUNK_ROWS = 32
STORES = 4
MESH = pl.DeviceIdType.MESH


def unpack_bits(words):
    shifts = jnp.arange(32, dtype=jnp.int32)
    bits = jnp.right_shift(words[:, :, None], shifts[None, None, :]) & 1
    return bits.reshape(words.shape[0], words.shape[1] * 32).astype(jnp.float32)


def rows_backward(grad_rows, input_rows, word_rows, gain):
    keep = unpack_bits(word_rows)
    dropped = input_rows.astype(jnp.float32) * keep * (1.0 / KEEP_RATE)
    inverse = lax.rsqrt(jnp.mean(dropped * dropped, axis=-1, keepdims=True) + EPSILON)
    normed = dropped * inverse
    grads = grad_rows.astype(jnp.float32)
    scaled = gain[None, :] * grads
    centre = jnp.mean(scaled * normed, axis=-1, keepdims=True)
    grad_in = (inverse * (scaled - normed * centre) * keep * (1.0 / KEEP_RATE)).astype(jnp.bfloat16)
    partial_sum = jnp.sum(grads * normed, axis=0)
    return (grad_in, partial_sum)


def plain(grad_out, saved_input, keep_bits, gain):
    groups = lax.axis_size("ba")
    rows = grad_out.shape[0] // groups
    pieces = grad_out.reshape(groups, rows, grad_out.shape[1])
    arrived = lax.all_to_all(pieces, "ba", split_axis=0, concat_axis=2, tiled=True)
    grad_rows = arrived.reshape(rows, arrived.shape[2])
    grad_in, partial_sum = rows_backward(grad_rows, saved_input, keep_bits, gain)
    total_tokens = rows * groups * lax.axis_size("aa")
    owned = lax.psum_scatter(partial_sum, "ba", scatter_dimension=0, tiled=True)
    share = lax.psum(owned, "aa")
    gain_grad = share * (1.0 / math.sqrt(total_tokens))
    return (grad_in, gain_grad)


def far_count(n_ba):
    return max(1, n_ba // 4)


def kernel(n_ba, n_aa, grad_hbm, input_hbm, bits_hbm, gain_hbm, out_ref, share_ref,
           staged, arrived, held, words, gain_ref, normed, masked_gain, outer, totals, sums,
           parts, slices, shares, far_shares, stage_sem, load_sem, near_send, near_recv,
           far_send, far_recv, part_send, part_recv, share_send, share_recv,
           late_send, late_recv, ready):
    ba, aa = lax.axis_index("ba"), lax.axis_index("aa")
    rows, width = arrived.shape[1], arrived.shape[2]
    depth = n_ba * width
    chunks = rows // CHUNK_ROWS
    tiles = width // LANES
    n_far = far_count(n_ba)
    far = list(range(n_ba - n_far, n_ba))
    near = list(range(1, n_ba - n_far))
    near_order = sorted(near, key=lambda step: (step == 1, step % 2))

    def column(step):
        return lax.rem(aa + step, n_aa)

    def column_source(step):
        return lax.rem(aa + n_aa - step, n_aa)

    def rows_of(chunk):
        start = chunk * CHUNK_ROWS
        if not isinstance(start, int):
            start = pl.multiple_of(start, CHUNK_ROWS)
        return pl.ds(start, CHUNK_ROWS)

    def stage(step):
        first = pl.ds(pl.multiple_of((ba ^ step) * rows, CHUNK_ROWS), rows)
        target = staged.at[step] if step else arrived.at[0]
        return pltpu.make_async_copy(grad_hbm.at[first], target, stage_sem.at[step])

    def near_piece(step):
        return pltpu.make_async_remote_copy(
            src_ref=staged.at[step], dst_ref=arrived.at[step],
            send_sem=near_send.at[step], recv_sem=near_recv.at[step],
            device_id={"ba": ba ^ step}, device_id_type=MESH,
        )

    def far_piece(chunk, index):
        step, block = far[index], rows_of(chunk)
        return pltpu.make_async_remote_copy(
            src_ref=staged.at[step, block], dst_ref=arrived.at[step, block],
            send_sem=far_send.at[chunk, index], recv_sem=far_recv.at[chunk, index],
            device_id={"ba": ba ^ step}, device_id_type=MESH,
        )

    def part(step):
        return pltpu.make_async_remote_copy(
            src_ref=parts.at[step], dst_ref=slices.at[step],
            send_sem=part_send.at[step], recv_sem=part_recv.at[step],
            device_id={"ba": ba ^ step}, device_id_type=MESH,
        )

    def share(step, slot):
        return pltpu.make_async_remote_copy(
            src_ref=shares.at[aa], dst_ref=shares.at[slot],
            send_sem=share_send.at[step], recv_sem=share_recv.at[step],
            device_id={"aa": column(step)}, device_id_type=MESH,
        )

    def late(step, index, slot):
        return pltpu.make_async_remote_copy(
            src_ref=parts.at[far[index]], dst_ref=far_shares.at[slot, index],
            send_sem=late_send.at[step, index], recv_sem=late_recv.at[step, index],
            device_id={"aa": column(step), "ba": ba ^ far[index]}, device_id_type=MESH,
        )

    barrier = pltpu.get_barrier_semaphore()
    for step in range(1, n_ba):
        pl.semaphore_signal(barrier, inc=1, device_id={"ba": ba ^ step}, device_id_type=MESH)
    for step in range(1, n_aa):
        pl.semaphore_signal(barrier, inc=1, device_id={"aa": column(step)}, device_id_type=MESH)
    for step in near_order:
        stage(step).start()
    loads = [
        pltpu.make_async_copy(bits_hbm, words, load_sem.at[0]),
        pltpu.make_async_copy(gain_hbm, gain_ref, load_sem.at[1]),
        pltpu.make_async_copy(input_hbm, held, load_sem.at[2]),
    ]
    for load in loads:
        load.start()
    for step in far + [0]:
        stage(step).start()
    pl.semaphore_wait(barrier, n_ba + n_aa - 2)
    for step in near_order:
        stage(step).wait()
        near_piece(step).start()
    for step in far:
        pl.semaphore_signal(ready, inc=1, device_id={"ba": ba ^ step}, device_id_type=MESH)
        stage(step).wait()
    ahead = chunks // 2
    for chunk in range(ahead):
        for index in range(n_far):
            far_piece(chunk, index).start()
    for load in loads:
        load.wait()

    lane = lax.broadcasted_iota(jnp.int32, (CHUNK_ROWS, LANES), 1)
    word_of = lane // 32
    flag = jnp.left_shift(jnp.int32(1), lane % 32)

    def span(source, tile):
        return pl.ds(pl.multiple_of(source * width + tile * LANES, LANES), LANES)

    def prepare(chunk, carry):
        block = rows_of(chunk)

        def drop(source, squares):
            row_words = words[block, :]
            for tile in range(tiles):
                at = span(source, tile)
                index = word_of + (source * tiles + tile) * (LANES // 32)
                spread = jnp.take_along_axis(row_words, index, axis=1, mode="promise_in_bounds")
                kept = (spread & flag) != 0
                dropped = jnp.where(kept, held[block, at].astype(jnp.float32), 0.0) * (1.0 / KEEP_RATE)
                normed[block, at] = dropped
                masked_gain[block, at] = jnp.where(kept, gain_ref[:, at], 0.0)
                squares = squares + dropped * dropped
            return squares

        squares = lax.fori_loop(0, n_ba, drop, jnp.zeros((CHUNK_ROWS, LANES), jnp.float32))
        mean = jnp.sum(squares, axis=1, keepdims=True) * (1.0 / depth)
        inverse = lax.rsqrt(mean + EPSILON)
        outer[block, :] = jnp.broadcast_to(inverse * (1.0 / KEEP_RATE), (CHUNK_ROWS, LANES))

        def scale(source, none):
            for tile in range(tiles):
                at = span(source, tile)
                normed[block, at] = normed[block, at] * inverse
            return none

        lax.fori_loop(0, n_ba, scale, 0)
        return carry

    lax.fori_loop(0, chunks, prepare, 0)
    sums[...] = jnp.zeros_like(sums)
    totals[...] = jnp.zeros_like(totals)

    def first(step, chunk):
        block, source = rows_of(chunk), ba ^ step
        total = totals[block, :]
        for tile in range(tiles):
            at = span(source, tile)
            here = slice(tile * LANES, (tile + 1) * LANES)
            grads = arrived[step, block, here].astype(jnp.float32)
            product = grads * normed[block, at]
            total = total + product * gain_ref[:, at]
            sums[step, :, here] += jnp.sum(product.reshape(CHUNK_ROWS // 8, 8, LANES), axis=0)
        totals[block, :] = total

    def finish(chunk):
        block = rows_of(chunk)
        factor = outer[block, :]
        centre = jnp.sum(totals[block, :], axis=1, keepdims=True) * (1.0 / depth)

        def last(step, none):
            for tile in range(tiles):
                at = span(ba ^ step, tile)
                grads = arrived[step, block, tile * LANES:(tile + 1) * LANES].astype(jnp.float32)
                value = factor * (masked_gain[block, at] * grads - normed[block, at] * centre)
                out_ref[block, at] = value.astype(jnp.bfloat16)
            return none

        lax.fori_loop(0, n_ba, last, 0)

    def fold(step):
        return jnp.sum(sums[step], axis=0, keepdims=True)

    for step in [0] + sorted(near, key=lambda step: (step != 1, step % 2)):
        if step:
            near_piece(step).wait_recv()
        else:
            stage(0).wait()

        def whole(chunk, none, step=step):
            first(step, chunk)
            return none

        lax.fori_loop(0, chunks, whole, 0)
        if step:
            parts[step] = fold(step)
        else:
            slices[0] = fold(0)
    for step in reversed(near):
        part(step).start()
    for chunk in range(ahead, chunks):
        for index in range(n_far):
            far_piece(chunk, index).start()

    def gather_near():
        total = slices[0]
        for step in near:
            part(step).wait_recv()
            total = total + slices[step]
        shares[aa] = total
        for step in range(1, n_aa):
            share(step, aa).start()

    for chunk in range(chunks):
        if chunk == chunks - 1:
            gather_near()
        for index in range(n_far):
            far_piece(chunk, index).wait_recv()
            first(far[index], chunk)
        if chunk < chunks - 1:
            finish(chunk)
    for step in far:
        parts[step] = fold(step)
    pl.semaphore_wait(ready, n_far)
    for step in reversed(range(n_aa)):
        for index in range(n_far):
            late(step, index, aa).start()
    finish(chunks - 1)
    for step in near:
        near_piece(step).wait_send()
        part(step).wait_send()
    for chunk in range(chunks):
        for index in range(n_far):
            far_piece(chunk, index).wait_send()
    for step in range(1, n_aa):
        share(step, column_source(step)).wait_recv()
    for step in range(n_aa):
        for index in range(n_far):
            late(step, index, column_source(step)).wait_recv()
    total = jnp.zeros((1, width), jnp.float32)
    for source in range(n_aa):
        total = total + shares[source]
        for index in range(n_far):
            total = total + far_shares[source, index]
    share_ref[...] = total * (1.0 / math.sqrt(rows * n_ba * n_aa))
    for step in range(1, n_aa):
        share(step, aa).wait_send()
    for step in range(n_aa):
        for index in range(n_far):
            late(step, index, aa).wait_send()


def store(grad_vmem, share_vmem, grad_hbm, share_hbm, sem):
    rows = grad_vmem.shape[0] // STORES
    copies = [pltpu.make_async_copy(share_vmem, share_hbm, sem.at[STORES])]
    for index in range(STORES):
        block = pl.ds(index * rows, rows)
        copies.append(pltpu.make_async_copy(grad_vmem.at[block], grad_hbm.at[block], sem.at[index]))
    for copy in copies:
        copy.start()
    for copy in copies:
        copy.wait()


def fused(grad_out, saved_input, keep_bits, gain):
    n_ba, n_aa = lax.axis_size("ba"), lax.axis_size("aa")
    width = grad_out.shape[1]
    rows, depth = saved_input.shape
    chunks, n_far = rows // CHUNK_ROWS, far_count(n_ba)
    f32 = jnp.float32
    grad_in, share = pl.pallas_call(
        functools.partial(kernel, n_ba, n_aa),
        out_shape=(
            pltpu.VMEM((rows, depth), jnp.bfloat16),
            pltpu.VMEM((1, width), f32),
        ),
        in_specs=[pl.BlockSpec(memory_space=pl.ANY)] * 4,
        out_specs=(pl.BlockSpec(memory_space=pltpu.VMEM), pl.BlockSpec(memory_space=pltpu.VMEM)),
        scratch_shapes=[
            pltpu.VMEM((n_ba, rows, width), jnp.bfloat16),
            pltpu.VMEM((n_ba, rows, width), jnp.bfloat16),
            pltpu.VMEM((rows, depth), jnp.bfloat16),
            pltpu.VMEM(keep_bits.shape, jnp.int32),
            pltpu.VMEM((1, depth), f32),
            pltpu.VMEM((rows, depth), f32),
            pltpu.VMEM((rows, depth), f32),
            pltpu.VMEM((rows, LANES), f32),
            pltpu.VMEM((rows, LANES), f32),
            pltpu.VMEM((n_ba, 8, width), f32),
            pltpu.VMEM((n_ba, 1, width), f32),
            pltpu.VMEM((n_ba, 1, width), f32),
            pltpu.VMEM((n_aa, 1, width), f32),
            pltpu.VMEM((n_aa, n_far, 1, width), f32),
            pltpu.SemaphoreType.DMA((n_ba,)),
            pltpu.SemaphoreType.DMA((3,)),
            pltpu.SemaphoreType.DMA((n_ba,)),
            pltpu.SemaphoreType.DMA((n_ba,)),
            pltpu.SemaphoreType.DMA((chunks, n_far)),
            pltpu.SemaphoreType.DMA((chunks, n_far)),
            pltpu.SemaphoreType.DMA((n_ba,)),
            pltpu.SemaphoreType.DMA((n_ba,)),
            pltpu.SemaphoreType.DMA((n_aa,)),
            pltpu.SemaphoreType.DMA((n_aa,)),
            pltpu.SemaphoreType.DMA((n_aa, n_far)),
            pltpu.SemaphoreType.DMA((n_aa, n_far)),
            pltpu.SemaphoreType.REGULAR,
        ],
        compiler_params=pltpu.CompilerParams(collective_id=0, has_side_effects=True),
        name="regroup_backward",
    )(grad_out, saved_input, keep_bits, gain.reshape(1, depth))
    grad_in, share = pl.pallas_call(
        store,
        out_shape=(
            jax.ShapeDtypeStruct((rows, depth), jnp.bfloat16),
            jax.ShapeDtypeStruct((1, width), f32),
        ),
        in_specs=[pl.BlockSpec(memory_space=pltpu.VMEM)] * 2,
        out_specs=[pl.BlockSpec(memory_space=pl.ANY)] * 2,
        scratch_shapes=[pltpu.SemaphoreType.DMA((STORES + 1,))],
        name="store_results",
    )(*(pltpu.with_memory_space_constraint(x, pltpu.VMEM) for x in (grad_in, share)))
    return (grad_in, share.reshape(width))


def per_device(grad_out, saved_input, keep_bits, gain):
    fits = grad_out.shape[1] % LANES == 0 and saved_input.shape[0] % CHUNK_ROWS == 0
    fits = fits and keep_bits.shape[1] == LANES
    n_ba = lax.axis_size("ba")
    fits = fits and n_ba > 1 and n_ba & (n_ba - 1) == 0
    body = fused if fits else plain
    return body(grad_out, saved_input, keep_bits, gain)


def solution(mesh):
    placed = (P("aa", "ba"), P(("aa", "ba"), None), P(("aa", "ba"), None), P())
    return jax.shard_map(
        per_device,
        mesh=mesh,
        in_specs=placed,
        out_specs=(P(("aa", "ba"), None), P("ba")),
        check_vma=False,
    )
```

```python
import functools
import math

import jax
import jax.numpy as jnp
from jax import lax
from jax.experimental import pallas as pl
from jax.experimental.pallas import tpu as pltpu
from jax.sharding import PartitionSpec as P

KEEP_RATE = 0.9
EPSILON = 1e-06
LANES = 128
CHUNK_ROWS = 32
STORES = 4
MESH = pl.DeviceIdType.MESH


def unpack_bits(words):
    shifts = jnp.arange(32, dtype=jnp.int32)
    bits = jnp.right_shift(words[:, :, None], shifts[None, None, :]) & 1
    return bits.reshape(words.shape[0], words.shape[1] * 32).astype(jnp.float32)


def rows_backward(grad_rows, input_rows, word_rows, gain):
    keep = unpack_bits(word_rows)
    dropped = input_rows.astype(jnp.float32) * keep * (1.0 / KEEP_RATE)
    inverse = lax.rsqrt(jnp.mean(dropped * dropped, axis=-1, keepdims=True) + EPSILON)
    normed = dropped * inverse
    grads = grad_rows.astype(jnp.float32)
    scaled = gain[None, :] * grads
    centre = jnp.mean(scaled * normed, axis=-1, keepdims=True)
    grad_in = (inverse * (scaled - normed * centre) * keep * (1.0 / KEEP_RATE)).astype(jnp.bfloat16)
    partial_sum = jnp.sum(grads * normed, axis=0)
    return (grad_in, partial_sum)


def plain(grad_out, saved_input, keep_bits, gain):
    groups = lax.axis_size("ba")
    rows = grad_out.shape[0] // groups
    pieces = grad_out.reshape(groups, rows, grad_out.shape[1])
    arrived = lax.all_to_all(pieces, "ba", split_axis=0, concat_axis=2, tiled=True)
    grad_rows = arrived.reshape(rows, arrived.shape[2])
    grad_in, partial_sum = rows_backward(grad_rows, saved_input, keep_bits, gain)
    total_tokens = rows * groups * lax.axis_size("aa")
    owned = lax.psum_scatter(partial_sum, "ba", scatter_dimension=0, tiled=True)
    share = lax.psum(owned, "aa")
    gain_grad = share * (1.0 / math.sqrt(total_tokens))
    return (grad_in, gain_grad)


def late_steps(n_ba):
    return list(range(max(1, n_ba // 4), n_ba - n_ba // 4))


def kernel(n_ba, n_aa, grad_hbm, input_hbm, bits_hbm, gain_hbm, out_ref, share_ref,
           staged, arrived, held, words, gain_ref, normed, masked_gain, outer, totals, sums,
           parts, slices, shares, far_shares, stage_sem, load_sem, near_send, near_recv,
           far_send, far_recv, part_send, part_recv, share_send, share_recv,
           late_send, late_recv, ready):
    ba, aa = lax.axis_index("ba"), lax.axis_index("aa")
    rows, width = arrived.shape[1], arrived.shape[2]
    depth = n_ba * width
    chunks = rows // CHUNK_ROWS
    tiles = width // LANES
    far = late_steps(n_ba)
    far = sorted(far, key=lambda step: step % 2)
    n_far = len(far)
    near = [step for step in range(1, n_ba) if step not in far]
    near_order = sorted(near, reverse=True)

    def column(step):
        return lax.rem(aa + step, n_aa)

    def column_source(step):
        return lax.rem(aa + n_aa - step, n_aa)

    def rows_of(chunk):
        start = chunk * CHUNK_ROWS
        if not isinstance(start, int):
            start = pl.multiple_of(start, CHUNK_ROWS)
        return pl.ds(start, CHUNK_ROWS)

    def stage(step):
        first = pl.ds(pl.multiple_of((ba ^ step) * rows, CHUNK_ROWS), rows)
        target = staged.at[step] if step else arrived.at[0]
        return pltpu.make_async_copy(grad_hbm.at[first], target, stage_sem.at[step])

    def near_piece(step):
        return pltpu.make_async_remote_copy(
            src_ref=staged.at[step], dst_ref=arrived.at[step],
            send_sem=near_send.at[step], recv_sem=near_recv.at[step],
            device_id={"ba": ba ^ step}, device_id_type=MESH,
        )

    def far_piece(chunk, index):
        step, block = far[index], rows_of(chunk)
        return pltpu.make_async_remote_copy(
            src_ref=staged.at[step, block], dst_ref=arrived.at[step, block],
            send_sem=far_send.at[chunk, index], recv_sem=far_recv.at[chunk, index],
            device_id={"ba": ba ^ step}, device_id_type=MESH,
        )

    def part(step):
        return pltpu.make_async_remote_copy(
            src_ref=parts.at[step], dst_ref=slices.at[step],
            send_sem=part_send.at[step], recv_sem=part_recv.at[step],
            device_id={"ba": ba ^ step}, device_id_type=MESH,
        )

    def share(step, slot):
        return pltpu.make_async_remote_copy(
            src_ref=shares.at[aa], dst_ref=shares.at[slot],
            send_sem=share_send.at[step], recv_sem=share_recv.at[step],
            device_id={"aa": column(step)}, device_id_type=MESH,
        )

    def late(step, index, slot):
        return pltpu.make_async_remote_copy(
            src_ref=parts.at[far[index]], dst_ref=far_shares.at[slot, index],
            send_sem=late_send.at[step, index], recv_sem=late_recv.at[step, index],
            device_id={"aa": column(step), "ba": ba ^ far[index]}, device_id_type=MESH,
        )

    barrier = pltpu.get_barrier_semaphore()
    for step in range(1, n_ba):
        pl.semaphore_signal(barrier, inc=1, device_id={"ba": ba ^ step}, device_id_type=MESH)
    for step in range(1, n_aa):
        pl.semaphore_signal(barrier, inc=1, device_id={"aa": column(step)}, device_id_type=MESH)
    for step in near_order:
        stage(step).start()
    loads = [
        pltpu.make_async_copy(bits_hbm, words, load_sem.at[0]),
        pltpu.make_async_copy(gain_hbm, gain_ref, load_sem.at[1]),
        pltpu.make_async_copy(input_hbm, held, load_sem.at[2]),
    ]
    for load in loads:
        load.start()
    for step in far + [0]:
        stage(step).start()
    pl.semaphore_wait(barrier, n_ba + n_aa - 2)
    for step in near_order:
        stage(step).wait()
        near_piece(step).start()
    for step in far:
        pl.semaphore_signal(ready, inc=1, device_id={"ba": ba ^ step}, device_id_type=MESH)
        stage(step).wait()
    for load in loads:
        load.wait()

    lane = lax.broadcasted_iota(jnp.int32, (CHUNK_ROWS, LANES), 1)
    word_of = lane // 32
    flag = jnp.left_shift(jnp.int32(1), lane % 32)

    def span(source, tile):
        return pl.ds(pl.multiple_of(source * width + tile * LANES, LANES), LANES)

    def prepare(chunk, carry):
        block = rows_of(chunk)

        def drop(source, squares):
            row_words = words[block, :]
            for tile in range(tiles):
                at = span(source, tile)
                index = word_of + (source * tiles + tile) * (LANES // 32)
                spread = jnp.take_along_axis(row_words, index, axis=1, mode="promise_in_bounds")
                kept = (spread & flag) != 0
                dropped = jnp.where(kept, held[block, at].astype(jnp.float32), 0.0) * (1.0 / KEEP_RATE)
                normed[block, at] = dropped
                masked_gain[block, at] = jnp.where(kept, gain_ref[:, at], 0.0)
                squares = squares + dropped * dropped
            return squares

        squares = lax.fori_loop(0, n_ba, drop, jnp.zeros((CHUNK_ROWS, LANES), jnp.float32))
        mean = jnp.sum(squares, axis=1, keepdims=True) * (1.0 / depth)
        inverse = lax.rsqrt(mean + EPSILON)
        outer[block, :] = jnp.broadcast_to(inverse * (1.0 / KEEP_RATE), (CHUNK_ROWS, LANES))

        def scale(source, none):
            for tile in range(tiles):
                at = span(source, tile)
                normed[block, at] = normed[block, at] * inverse
            return none

        lax.fori_loop(0, n_ba, scale, 0)
        return carry

    lax.fori_loop(0, chunks, prepare, 0)
    sums[...] = jnp.zeros_like(sums)
    totals[...] = jnp.zeros_like(totals)
    for step in near:
        near_piece(step).wait_send()
    ahead = chunks // 2
    for chunk in range(ahead):
        for index in range(n_far):
            far_piece(chunk, index).start()

    def first(step, chunk):
        block, source = rows_of(chunk), ba ^ step
        total = totals[block, :]
        for tile in range(tiles):
            at = span(source, tile)
            here = slice(tile * LANES, (tile + 1) * LANES)
            grads = arrived[step, block, here].astype(jnp.float32)
            product = grads * normed[block, at]
            total = total + product * gain_ref[:, at]
            sums[step, :, here] += jnp.sum(product.reshape(CHUNK_ROWS // 8, 8, LANES), axis=0)
        totals[block, :] = total

    def finish(chunk):
        block = rows_of(chunk)
        factor = outer[block, :]
        centre = jnp.sum(totals[block, :], axis=1, keepdims=True) * (1.0 / depth)

        def last(step, none):
            for tile in range(tiles):
                at = span(ba ^ step, tile)
                grads = arrived[step, block, tile * LANES:(tile + 1) * LANES].astype(jnp.float32)
                value = factor * (masked_gain[block, at] * grads - normed[block, at] * centre)
                out_ref[block, at] = value.astype(jnp.bfloat16)
            return none

        lax.fori_loop(0, n_ba, last, 0)

    def fold(step):
        return jnp.sum(sums[step], axis=0, keepdims=True)

    for step in [0] + near:
        if step:
            near_piece(step).wait_recv()
        else:
            stage(0).wait()

        def whole(chunk, none, step=step):
            first(step, chunk)
            return none

        lax.fori_loop(0, chunks, whole, 0)
        if step:
            parts[step] = fold(step)
        else:
            slices[0] = fold(0)
    for step in reversed(near):
        part(step).start()
    for chunk in range(ahead, chunks):
        for index in range(n_far):
            far_piece(chunk, index).start()

    def gather_near():
        total = slices[0]
        for step in near:
            part(step).wait_recv()
            total = total + slices[step]
        shares[aa] = total
        for step in range(1, n_aa):
            share(step, aa).start()

    for chunk in range(chunks):
        if chunk == chunks - 1:
            gather_near()
        for index in range(n_far):
            far_piece(chunk, index).wait_recv()
            first(far[index], chunk)
        if chunk < chunks - 1:
            finish(chunk)
    for step in far:
        parts[step] = fold(step)
    pl.semaphore_wait(ready, n_far)
    for step in reversed(range(n_aa)):
        for index in range(n_far):
            late(step, index, aa).start()
    finish(chunks - 1)
    for step in near:
        part(step).wait_send()
    for chunk in range(chunks):
        for index in range(n_far):
            far_piece(chunk, index).wait_send()
    for step in range(1, n_aa):
        share(step, column_source(step)).wait_recv()
    for step in range(n_aa):
        for index in range(n_far):
            late(step, index, column_source(step)).wait_recv()
    total = jnp.zeros((1, width), jnp.float32)
    for source in range(n_aa):
        total = total + shares[source]
        for index in range(n_far):
            total = total + far_shares[source, index]
    share_ref[...] = total * (1.0 / math.sqrt(rows * n_ba * n_aa))
    for step in range(1, n_aa):
        share(step, aa).wait_send()
    for step in range(n_aa):
        for index in range(n_far):
            late(step, index, aa).wait_send()


def store(grad_vmem, share_vmem, grad_hbm, share_hbm, sem):
    rows = grad_vmem.shape[0] // STORES
    copies = [pltpu.make_async_copy(share_vmem, share_hbm, sem.at[STORES])]
    for index in range(STORES):
        block = pl.ds(index * rows, rows)
        copies.append(pltpu.make_async_copy(grad_vmem.at[block], grad_hbm.at[block], sem.at[index]))
    for copy in copies:
        copy.start()
    for copy in copies:
        copy.wait()


def fused(grad_out, saved_input, keep_bits, gain):
    n_ba, n_aa = lax.axis_size("ba"), lax.axis_size("aa")
    width = grad_out.shape[1]
    rows, depth = saved_input.shape
    chunks, n_far = rows // CHUNK_ROWS, len(late_steps(n_ba))
    f32 = jnp.float32
    grad_in, share = pl.pallas_call(
        functools.partial(kernel, n_ba, n_aa),
        out_shape=(
            pltpu.VMEM((rows, depth), jnp.bfloat16),
            pltpu.VMEM((1, width), f32),
        ),
        in_specs=[pl.BlockSpec(memory_space=pl.ANY)] * 4,
        out_specs=(pl.BlockSpec(memory_space=pltpu.VMEM), pl.BlockSpec(memory_space=pltpu.VMEM)),
        scratch_shapes=[
            pltpu.VMEM((n_ba, rows, width), jnp.bfloat16),
            pltpu.VMEM((n_ba, rows, width), jnp.bfloat16),
            pltpu.VMEM((rows, depth), jnp.bfloat16),
            pltpu.VMEM(keep_bits.shape, jnp.int32),
            pltpu.VMEM((1, depth), f32),
            pltpu.VMEM((rows, depth), f32),
            pltpu.VMEM((rows, depth), f32),
            pltpu.VMEM((rows, LANES), f32),
            pltpu.VMEM((rows, LANES), f32),
            pltpu.VMEM((n_ba, 8, width), f32),
            pltpu.VMEM((n_ba, 1, width), f32),
            pltpu.VMEM((n_ba, 1, width), f32),
            pltpu.VMEM((n_aa, 1, width), f32),
            pltpu.VMEM((n_aa, n_far, 1, width), f32),
            pltpu.SemaphoreType.DMA((n_ba,)),
            pltpu.SemaphoreType.DMA((3,)),
            pltpu.SemaphoreType.DMA((n_ba,)),
            pltpu.SemaphoreType.DMA((n_ba,)),
            pltpu.SemaphoreType.DMA((chunks, n_far)),
            pltpu.SemaphoreType.DMA((chunks, n_far)),
            pltpu.SemaphoreType.DMA((n_ba,)),
            pltpu.SemaphoreType.DMA((n_ba,)),
            pltpu.SemaphoreType.DMA((n_aa,)),
            pltpu.SemaphoreType.DMA((n_aa,)),
            pltpu.SemaphoreType.DMA((n_aa, n_far)),
            pltpu.SemaphoreType.DMA((n_aa, n_far)),
            pltpu.SemaphoreType.REGULAR,
        ],
        compiler_params=pltpu.CompilerParams(collective_id=0, has_side_effects=True),
        name="regroup_backward",
    )(grad_out, saved_input, keep_bits, gain.reshape(1, depth))
    grad_in, share = pl.pallas_call(
        store,
        out_shape=(
            jax.ShapeDtypeStruct((rows, depth), jnp.bfloat16),
            jax.ShapeDtypeStruct((1, width), f32),
        ),
        in_specs=[pl.BlockSpec(memory_space=pltpu.VMEM)] * 2,
        out_specs=[pl.BlockSpec(memory_space=pl.ANY)] * 2,
        scratch_shapes=[pltpu.SemaphoreType.DMA((STORES + 1,))],
        name="store_results",
    )(*(pltpu.with_memory_space_constraint(x, pltpu.VMEM) for x in (grad_in, share)))
    return (grad_in, share.reshape(width))


def per_device(grad_out, saved_input, keep_bits, gain):
    fits = grad_out.shape[1] % LANES == 0 and saved_input.shape[0] % CHUNK_ROWS == 0
    fits = fits and keep_bits.shape[1] == LANES
    n_ba = lax.axis_size("ba")
    fits = fits and n_ba > 1 and n_ba & (n_ba - 1) == 0
    body = fused if fits else plain
    return body(grad_out, saved_input, keep_bits, gain)


def solution(mesh):
    placed = (P("aa", "ba"), P(("aa", "ba"), None), P(("aa", "ba"), None), P())
    return jax.shard_map(
        per_device,
        mesh=mesh,
        in_specs=placed,
        out_specs=(P(("aa", "ba"), None), P("ba")),
        check_vma=False,
    )
```

```python
import functools
import math

import jax
import jax.numpy as jnp
from jax import lax
from jax.experimental import pallas as pl
from jax.experimental.pallas import tpu as pltpu
from jax.sharding import PartitionSpec as P

KEEP_RATE = 0.9
EPSILON = 1e-06
LANES = 128
CHUNK_ROWS = 64
STORES = 4
MESH = pl.DeviceIdType.MESH


def unpack_bits(words):
    shifts = jnp.arange(32, dtype=jnp.int32)
    bits = jnp.right_shift(words[:, :, None], shifts[None, None, :]) & 1
    return bits.reshape(words.shape[0], words.shape[1] * 32).astype(jnp.float32)


def rows_backward(grad_rows, input_rows, word_rows, gain):
    keep = unpack_bits(word_rows)
    dropped = input_rows.astype(jnp.float32) * keep * (1.0 / KEEP_RATE)
    inverse = lax.rsqrt(jnp.mean(dropped * dropped, axis=-1, keepdims=True) + EPSILON)
    normed = dropped * inverse
    grads = grad_rows.astype(jnp.float32)
    scaled = gain[None, :] * grads
    centre = jnp.mean(scaled * normed, axis=-1, keepdims=True)
    grad_in = (inverse * (scaled - normed * centre) * keep * (1.0 / KEEP_RATE)).astype(jnp.bfloat16)
    partial_sum = jnp.sum(grads * normed, axis=0)
    return (grad_in, partial_sum)


def plain(grad_out, saved_input, keep_bits, gain):
    groups = lax.axis_size("ba")
    rows = grad_out.shape[0] // groups
    pieces = grad_out.reshape(groups, rows, grad_out.shape[1])
    arrived = lax.all_to_all(pieces, "ba", split_axis=0, concat_axis=2, tiled=True)
    grad_rows = arrived.reshape(rows, arrived.shape[2])
    grad_in, partial_sum = rows_backward(grad_rows, saved_input, keep_bits, gain)
    total_tokens = rows * groups * lax.axis_size("aa")
    owned = lax.psum_scatter(partial_sum, "ba", scatter_dimension=0, tiled=True)
    share = lax.psum(owned, "aa")
    gain_grad = share * (1.0 / math.sqrt(total_tokens))
    return (grad_in, gain_grad)


def late_steps(n_ba):
    return list(range(max(1, n_ba // 4), n_ba - n_ba // 4))


def kernel(n_ba, n_aa, grad_hbm, input_hbm, bits_hbm, gain_hbm, out_ref, share_ref,
           staged, arrived, held, words, gain_ref, normed, masked_gain, outer, totals, sums,
           parts, slices, shares, far_shares, stage_sem, load_sem, near_send, near_recv,
           far_send, far_recv, part_send, part_recv, share_send, share_recv,
           late_send, late_recv, ready):
    ba, aa = lax.axis_index("ba"), lax.axis_index("aa")
    rows, width = arrived.shape[1], arrived.shape[2]
    depth = n_ba * width
    chunks = rows // CHUNK_ROWS
    tiles = width // LANES
    far = late_steps(n_ba)
    far = sorted(far, key=lambda step: step % 2)
    n_far = len(far)
    near = [step for step in range(1, n_ba) if step not in far]
    near_order = sorted(near, reverse=True)

    def column(step):
        return lax.rem(aa + step, n_aa)

    def column_source(step):
        return lax.rem(aa + n_aa - step, n_aa)

    def rows_of(chunk):
        start = chunk * CHUNK_ROWS
        if not isinstance(start, int):
            start = pl.multiple_of(start, CHUNK_ROWS)
        return pl.ds(start, CHUNK_ROWS)

    def stage(step):
        first = pl.ds(pl.multiple_of((ba ^ step) * rows, CHUNK_ROWS), rows)
        target = staged.at[step] if step else arrived.at[0]
        return pltpu.make_async_copy(grad_hbm.at[first], target, stage_sem.at[step])

    def near_piece(step):
        return pltpu.make_async_remote_copy(
            src_ref=staged.at[step], dst_ref=arrived.at[step],
            send_sem=near_send.at[step], recv_sem=near_recv.at[step],
            device_id={"ba": ba ^ step}, device_id_type=MESH,
        )

    def far_piece(chunk, index):
        step, block = far[index], rows_of(chunk)
        return pltpu.make_async_remote_copy(
            src_ref=staged.at[step, block], dst_ref=arrived.at[step, block],
            send_sem=far_send.at[chunk, index], recv_sem=far_recv.at[chunk, index],
            device_id={"ba": ba ^ step}, device_id_type=MESH,
        )

    def part(step):
        return pltpu.make_async_remote_copy(
            src_ref=parts.at[step], dst_ref=slices.at[step],
            send_sem=part_send.at[step], recv_sem=part_recv.at[step],
            device_id={"ba": ba ^ step}, device_id_type=MESH,
        )

    def share(step, slot):
        return pltpu.make_async_remote_copy(
            src_ref=shares.at[aa], dst_ref=shares.at[slot],
            send_sem=share_send.at[step], recv_sem=share_recv.at[step],
            device_id={"aa": column(step)}, device_id_type=MESH,
        )

    def late(step, index, slot):
        return pltpu.make_async_remote_copy(
            src_ref=parts.at[far[index]], dst_ref=far_shares.at[slot, index],
            send_sem=late_send.at[step, index], recv_sem=late_recv.at[step, index],
            device_id={"aa": column(step), "ba": ba ^ far[index]}, device_id_type=MESH,
        )

    barrier = pltpu.get_barrier_semaphore()
    for step in range(1, n_ba):
        pl.semaphore_signal(barrier, inc=1, device_id={"ba": ba ^ step}, device_id_type=MESH)
    for step in range(1, n_aa):
        pl.semaphore_signal(barrier, inc=1, device_id={"aa": column(step)}, device_id_type=MESH)
    for step in near_order:
        stage(step).start()
    loads = [
        pltpu.make_async_copy(bits_hbm, words, load_sem.at[0]),
        pltpu.make_async_copy(gain_hbm, gain_ref, load_sem.at[1]),
        pltpu.make_async_copy(input_hbm, held, load_sem.at[2]),
    ]
    for load in loads:
        load.start()
    for step in far + [0]:
        stage(step).start()
    pl.semaphore_wait(barrier, n_ba + n_aa - 2)
    for step in near_order:
        stage(step).wait()
        near_piece(step).start()
    for step in far:
        pl.semaphore_signal(ready, inc=1, device_id={"ba": ba ^ step}, device_id_type=MESH)
        stage(step).wait()
    for load in loads:
        load.wait()

    lane = lax.broadcasted_iota(jnp.int32, (CHUNK_ROWS, LANES), 1)
    word_of = lane // 32
    flag = jnp.left_shift(jnp.int32(1), lane % 32)

    def span(source, tile):
        return pl.ds(pl.multiple_of(source * width + tile * LANES, LANES), LANES)

    def prepare(chunk, carry):
        block = rows_of(chunk)

        def drop(source, squares):
            row_words = words[block, :]
            for tile in range(tiles):
                at = span(source, tile)
                index = word_of + (source * tiles + tile) * (LANES // 32)
                spread = jnp.take_along_axis(row_words, index, axis=1, mode="promise_in_bounds")
                kept = (spread & flag) != 0
                dropped = jnp.where(kept, held[block, at].astype(jnp.float32), 0.0) * (1.0 / KEEP_RATE)
                normed[block, at] = dropped
                masked_gain[block, at] = jnp.where(kept, gain_ref[:, at], 0.0)
                squares = squares + dropped * dropped
            return squares

        squares = lax.fori_loop(0, n_ba, drop, jnp.zeros((CHUNK_ROWS, LANES), jnp.float32))
        mean = jnp.sum(squares, axis=1, keepdims=True) * (1.0 / depth)
        inverse = lax.rsqrt(mean + EPSILON)
        outer[block, :] = jnp.broadcast_to(inverse * (1.0 / KEEP_RATE), (CHUNK_ROWS, LANES))

        def scale(source, none):
            for tile in range(tiles):
                at = span(source, tile)
                normed[block, at] = normed[block, at] * inverse
            return none

        lax.fori_loop(0, n_ba, scale, 0)
        return carry

    lax.fori_loop(0, chunks, prepare, 0)
    sums[...] = jnp.zeros_like(sums)
    totals[...] = jnp.zeros_like(totals)
    for step in near:
        near_piece(step).wait_send()
    ahead = chunks // 2
    for chunk in range(ahead):
        for index in range(n_far):
            far_piece(chunk, index).start()

    def first(step, chunk):
        block, source = rows_of(chunk), ba ^ step
        total = totals[block, :]
        for tile in range(tiles):
            at = span(source, tile)
            here = slice(tile * LANES, (tile + 1) * LANES)
            grads = arrived[step, block, here].astype(jnp.float32)
            product = grads * normed[block, at]
            total = total + product * gain_ref[:, at]
            sums[step, :, here] += jnp.sum(product.reshape(CHUNK_ROWS // 8, 8, LANES), axis=0)
        totals[block, :] = total

    def finish(chunk):
        block = rows_of(chunk)
        factor = outer[block, :]
        centre = jnp.sum(totals[block, :], axis=1, keepdims=True) * (1.0 / depth)

        def last(step, none):
            for tile in range(tiles):
                at = span(ba ^ step, tile)
                grads = arrived[step, block, tile * LANES:(tile + 1) * LANES].astype(jnp.float32)
                value = factor * (masked_gain[block, at] * grads - normed[block, at] * centre)
                out_ref[block, at] = value.astype(jnp.bfloat16)
            return none

        lax.fori_loop(0, n_ba, last, 0)

    def fold(step):
        return jnp.sum(sums[step], axis=0, keepdims=True)

    for step in [0] + near:
        if step:
            near_piece(step).wait_recv()
        else:
            stage(0).wait()

        def whole(chunk, none, step=step):
            first(step, chunk)
            return none

        lax.fori_loop(0, chunks, whole, 0)
        if step:
            parts[step] = fold(step)
        else:
            slices[0] = fold(0)
    for step in reversed(near):
        part(step).start()
    for chunk in range(ahead, chunks):
        for index in range(n_far):
            far_piece(chunk, index).start()

    def gather_near():
        total = slices[0]
        for step in near:
            part(step).wait_recv()
            total = total + slices[step]
        shares[aa] = total
        for step in range(1, n_aa):
            share(step, aa).start()

    for chunk in range(chunks):
        if chunk == chunks - 1:
            gather_near()
        for index in range(n_far):
            far_piece(chunk, index).wait_recv()
            first(far[index], chunk)
        if chunk < chunks - 1:
            finish(chunk)
    for step in far:
        parts[step] = fold(step)
    pl.semaphore_wait(ready, n_far)
    for step in reversed(range(n_aa)):
        for index in range(n_far):
            late(step, index, aa).start()
    finish(chunks - 1)
    for step in near:
        part(step).wait_send()
    for chunk in range(chunks):
        for index in range(n_far):
            far_piece(chunk, index).wait_send()
    for step in range(1, n_aa):
        share(step, column_source(step)).wait_recv()
    for step in range(n_aa):
        for index in range(n_far):
            late(step, index, column_source(step)).wait_recv()
    total = jnp.zeros((1, width), jnp.float32)
    for source in range(n_aa):
        total = total + shares[source]
        for index in range(n_far):
            total = total + far_shares[source, index]
    share_ref[...] = total * (1.0 / math.sqrt(rows * n_ba * n_aa))
    for step in range(1, n_aa):
        share(step, aa).wait_send()
    for step in range(n_aa):
        for index in range(n_far):
            late(step, index, aa).wait_send()


def store(grad_vmem, share_vmem, grad_hbm, share_hbm, sem):
    rows = grad_vmem.shape[0] // STORES
    copies = [pltpu.make_async_copy(share_vmem, share_hbm, sem.at[STORES])]
    for index in range(STORES):
        block = pl.ds(index * rows, rows)
        copies.append(pltpu.make_async_copy(grad_vmem.at[block], grad_hbm.at[block], sem.at[index]))
    for copy in copies:
        copy.start()
    for copy in copies:
        copy.wait()


def fused(grad_out, saved_input, keep_bits, gain):
    n_ba, n_aa = lax.axis_size("ba"), lax.axis_size("aa")
    width = grad_out.shape[1]
    rows, depth = saved_input.shape
    chunks, n_far = rows // CHUNK_ROWS, len(late_steps(n_ba))
    f32 = jnp.float32
    grad_in, share = pl.pallas_call(
        functools.partial(kernel, n_ba, n_aa),
        out_shape=(
            pltpu.VMEM((rows, depth), jnp.bfloat16),
            pltpu.VMEM((1, width), f32),
        ),
        in_specs=[pl.BlockSpec(memory_space=pl.ANY)] * 4,
        out_specs=(pl.BlockSpec(memory_space=pltpu.VMEM), pl.BlockSpec(memory_space=pltpu.VMEM)),
        scratch_shapes=[
            pltpu.VMEM((n_ba, rows, width), jnp.bfloat16),
            pltpu.VMEM((n_ba, rows, width), jnp.bfloat16),
            pltpu.VMEM((rows, depth), jnp.bfloat16),
            pltpu.VMEM(keep_bits.shape, jnp.int32),
            pltpu.VMEM((1, depth), f32),
            pltpu.VMEM((rows, depth), f32),
            pltpu.VMEM((rows, depth), f32),
            pltpu.VMEM((rows, LANES), f32),
            pltpu.VMEM((rows, LANES), f32),
            pltpu.VMEM((n_ba, 8, width), f32),
            pltpu.VMEM((n_ba, 1, width), f32),
            pltpu.VMEM((n_ba, 1, width), f32),
            pltpu.VMEM((n_aa, 1, width), f32),
            pltpu.VMEM((n_aa, n_far, 1, width), f32),
            pltpu.SemaphoreType.DMA((n_ba,)),
            pltpu.SemaphoreType.DMA((3,)),
            pltpu.SemaphoreType.DMA((n_ba,)),
            pltpu.SemaphoreType.DMA((n_ba,)),
            pltpu.SemaphoreType.DMA((chunks, n_far)),
            pltpu.SemaphoreType.DMA((chunks, n_far)),
            pltpu.SemaphoreType.DMA((n_ba,)),
            pltpu.SemaphoreType.DMA((n_ba,)),
            pltpu.SemaphoreType.DMA((n_aa,)),
            pltpu.SemaphoreType.DMA((n_aa,)),
            pltpu.SemaphoreType.DMA((n_aa, n_far)),
            pltpu.SemaphoreType.DMA((n_aa, n_far)),
            pltpu.SemaphoreType.REGULAR,
        ],
        compiler_params=pltpu.CompilerParams(collective_id=0, has_side_effects=True),
        name="regroup_backward",
    )(grad_out, saved_input, keep_bits, gain.reshape(1, depth))
    grad_in, share = pl.pallas_call(
        store,
        out_shape=(
            jax.ShapeDtypeStruct((rows, depth), jnp.bfloat16),
            jax.ShapeDtypeStruct((1, width), f32),
        ),
        in_specs=[pl.BlockSpec(memory_space=pltpu.VMEM)] * 2,
        out_specs=[pl.BlockSpec(memory_space=pl.ANY)] * 2,
        scratch_shapes=[pltpu.SemaphoreType.DMA((STORES + 1,))],
        name="store_results",
    )(*(pltpu.with_memory_space_constraint(x, pltpu.VMEM) for x in (grad_in, share)))
    return (grad_in, share.reshape(width))


def per_device(grad_out, saved_input, keep_bits, gain):
    fits = grad_out.shape[1] % LANES == 0 and saved_input.shape[0] % CHUNK_ROWS == 0
    fits = fits and keep_bits.shape[1] == LANES
    n_ba = lax.axis_size("ba")
    fits = fits and n_ba > 1 and n_ba & (n_ba - 1) == 0
    body = fused if fits else plain
    return body(grad_out, saved_input, keep_bits, gain)


def solution(mesh):
    placed = (P("aa", "ba"), P(("aa", "ba"), None), P(("aa", "ba"), None), P())
    return jax.shard_map(
        per_device,
        mesh=mesh,
        in_specs=placed,
        out_specs=(P(("aa", "ba"), None), P("ba")),
        check_vma=False,
    )
```
